16 devices in a mesh: rep: 4 (over z, y), data: 4 (over x, core).
Axes of the slice: x: 2, y: 2, z: 2, core: 2. Of those that a mesh axis runs over, the one named last changes fastest.
Arguments:
- hidden: bfloat16 [8192, 3584], P(('rep', 'data')), parts along dimension 0
- adapter_id: int32 [8192], P(('rep', 'data')), parts along dimension 0
- w_gate: bfloat16 [3584, 18944], replicated
- w_up: bfloat16 [3584, 18944], replicated
- w_down: bfloat16 [18944, 3584], replicated
- a_gate: bfloat16 [128, 3584, 16], replicated
- b_gate: bfloat16 [128, 16, 18944], P('data')
- a_up: bfloat16 [128, 3584, 16], replicated
- b_up: bfloat16 [128, 16, 18944], P('data')
- a_down: bfloat16 [128, 18944, 16], replicated
- b_down: bfloat16 [128, 16, 3584], P('data')
Outputs:
- output: bfloat16 [8192, 3584], P(('rep', 'data')), parts along dimension 0
There are 4 independent parts. The reference program is written for one: setup_inputs(seed, part) draws one part's arguments, and reference() takes and returns one part's arrays. A program takes and returns all parts, laid end to end along the dimension named above; an argument that names none is the same for every part.
All inputs are finite; a program needn't handle non-finite values.
Results may differ from the reference program's by a relative error of at most 0.0073344.
Values are sent between devices in bfloat16 or wider.
A program may use at most 2.25 GiB of HBM per device.

```python
import jax
import jax.numpy as jnp
from jax import lax

D = 3584
FF = 18944
RANK = 16
ADAPTERS = 128
GROUP = 4
TOKENS_DEV = 512
TOKENS = 2048
CAP = 256
PER_OWNER = ADAPTERS // GROUP
ROW_BLOCK = min(64, TOKENS)
LORA_SCALE = 2.0


def draw_ids(key):
    key_hot, key_src, key_one, key_two = jax.random.split(key, 4)
    hot_owner = jax.random.randint(key_hot, (), 0, GROUP)

    def one_source(src_key):
        key_slot, key_order = jax.random.split(src_key)
        slot_order = jax.random.permutation(key_slot, (GROUP - 1) * (CAP - 1))
        extra_rank = slot_order[:TOKENS_DEV - CAP - GROUP + 1] // (CAP - 1)
        other_rank = jnp.concatenate([jnp.arange(GROUP - 1, dtype=jnp.int32), extra_rank.astype(jnp.int32)])
        other_owner = other_rank + (other_rank >= hot_owner).astype(jnp.int32)
        owner_ids = jnp.concatenate([jnp.full((CAP,), hot_owner, jnp.int32), other_owner])
        return jax.random.permutation(key_order, owner_ids)

    owner_ids = jax.vmap(one_source)(jax.random.split(key_src, GROUP)).reshape(TOKENS)
    pick_one = jax.random.randint(key_one, (TOKENS,), 0, PER_OWNER)
    pick_two = jax.random.randint(key_two, (TOKENS,), 0, PER_OWNER)
    return (owner_ids * PER_OWNER + jnp.minimum(pick_one, pick_two)).astype(jnp.int32)


def weight(key, shape, scale):
    return (jax.random.normal(key, shape, jnp.float32) * scale).astype(jnp.bfloat16)


def setup_inputs(seed: int = 0, part: int = 0) -> dict:
    base_key = jax.random.key(seed)
    part_key = jax.random.fold_in(base_key, part)
    key_rows, key_ids = jax.random.split(part_key)
    keys = jax.random.split(base_key, 9)
    return {
        'hidden': jax.random.normal(key_rows, (TOKENS, D), jnp.float32).astype(jnp.bfloat16),
        'adapter_id': draw_ids(key_ids),
        'w_gate': weight(keys[0], (D, FF), D ** -0.5),
        'w_up': weight(keys[1], (D, FF), D ** -0.5),
        'w_down': weight(keys[2], (FF, D), FF ** -0.5),
        'a_gate': weight(keys[3], (ADAPTERS, D, RANK), D ** -0.5),
        'b_gate': weight(keys[4], (ADAPTERS, RANK, FF), 0.15 * RANK ** -0.5),
        'a_up': weight(keys[5], (ADAPTERS, D, RANK), D ** -0.5),
        'b_up': weight(keys[6], (ADAPTERS, RANK, FF), 0.15 * RANK ** -0.5),
        'a_down': weight(keys[7], (ADAPTERS, FF, RANK), FF ** -0.5),
        'b_down': weight(keys[8], (ADAPTERS, RANK, D), 0.25 * RANK ** -0.5),
    }


def lora_delta(act_rows, a_rows, b_rows):
    low_rows = jnp.einsum('tk,tkr->tr', act_rows.astype(jnp.float32), a_rows.astype(jnp.float32)).astype(jnp.bfloat16)
    full_rows = jnp.einsum('tr,trm->tm', low_rows.astype(jnp.float32), b_rows.astype(jnp.float32))
    return (LORA_SCALE * full_rows).astype(jnp.bfloat16)


def reference(hidden, adapter_id, w_gate, w_up, w_down, a_gate, b_gate, a_up, b_up, a_down, b_down):
    def one_block(block):
        block_rows, block_ids = block
        gate_act = jnp.dot(block_rows, w_gate, preferred_element_type=jnp.float32) + lora_delta(block_rows, a_gate[block_ids], b_gate[block_ids]).astype(jnp.float32)
        up_act = jnp.dot(block_rows, w_up, preferred_element_type=jnp.float32) + lora_delta(block_rows, a_up[block_ids], b_up[block_ids]).astype(jnp.float32)
        hid_act = (jax.nn.silu(gate_act) * up_act).astype(jnp.bfloat16)
        down_act = jnp.dot(hid_act, w_down, preferred_element_type=jnp.float32) + lora_delta(hid_act, a_down[block_ids], b_down[block_ids]).astype(jnp.float32)
        return (block_rows.astype(jnp.float32) + down_act).astype(jnp.bfloat16)

    out_blocks = lax.map(one_block, (hidden.reshape(TOKENS // ROW_BLOCK, ROW_BLOCK, D), adapter_id.reshape(TOKENS // ROW_BLOCK, ROW_BLOCK)))
    return out_blocks.reshape(TOKENS, D)
```

```python
import functools

import jax
import jax.numpy as jnp
from jax import lax
from jax.experimental import pallas as pl
from jax.experimental.pallas import tpu as pltpu
from jax.sharding import PartitionSpec as P

LORA_SCALE = 2.0
F32 = jnp.float32
BF16 = jnp.bfloat16
NT = (((1,), (1,)), ((), ()))
VMEM_LIMIT = 62 * 1024 * 1024


def row_counts(tok):
    if tok == 512:
        return (256, 320, 352, 368, 416, 512)
    return (tok // 2, tok)


def per_row_count(rows_ref, counts, body):
    rows = rows_ref[0]
    below = 0
    for count in counts:
        pl.when((rows > below) & (rows <= count))(functools.partial(body, count))
        below = count


def whole(shape):
    zeros = (0,) * len(shape)
    return pl.BlockSpec(shape, lambda *_: zeros, pipeline_mode=pl.Buffered(1))


def low_kernel(counts, rank, info_ref, x_ref, lid_ref, ag_ref, au_ref, lg_ref, lu_ref):
    width = ag_ref.shape[0]
    block = pl.program_id(0)

    def body(m):
        column = block * width + lax.broadcasted_iota(jnp.int32, (m, width), 1)
        mine = (column // rank) == lid_ref[:m, :]
        for a_ref, l_ref in ((ag_ref, lg_ref), (au_ref, lu_ref)):
            low = lax.dot_general(x_ref[:m, :], a_ref[...], NT, preferred_element_type=F32)
            l_ref[:m, :] = jnp.where(mine, low, 0.0).astype(BF16)

    per_row_count(info_ref, counts, body)


def low_rows(info, x, lid, ag, au, own_rows, rank):
    tok, d = x.shape
    width = own_rows // 2
    counts = row_counts(tok)
    spec_a = pl.BlockSpec((width, d), lambda b, info: ((info[1] ^ (b // 2)) * 2 + b % 2, 0))
    spec_l = pl.BlockSpec((tok, width), lambda b, info: (0, b))
    return pl.pallas_call(
        functools.partial(low_kernel, counts, rank),
        grid_spec=pltpu.PrefetchScalarGridSpec(
            num_scalar_prefetch=1,
            grid=(4,),
            in_specs=[whole((tok, d)), whole((tok, 1)), spec_a, spec_a],
            out_specs=[spec_l, spec_l],
        ),
        out_shape=[jax.ShapeDtypeStruct((tok, 4 * width), BF16)] * 2,
        compiler_params=pltpu.CompilerParams(vmem_limit_bytes=VMEM_LIMIT),
        cost_estimate=pl.CostEstimate(flops=2 * 2 * tok * d * 4 * width, bytes_accessed=4 * 4 * width * d, transcendentals=0),
    )(info, x, lid, ag, au)


def up_kernel(counts, sub, info_ref, x_ref, lg_ref, lu_ref, wg_ref, wu_ref, bg0_ref, bg1_ref, bu0_ref, bu1_ref, h_ref):
    half = bg0_ref.shape[0]

    def body(m):
        def columns(step, carry):
            at = pl.ds(pl.multiple_of(step * sub, sub), sub)

            def branch(w_ref, l_ref, b0_ref, b1_ref):
                base = jnp.dot(x_ref[:m, :], w_ref[:, at], preferred_element_type=F32)
                delta = jnp.dot(l_ref[:m, :half], b0_ref[:, at], preferred_element_type=F32)
                delta += jnp.dot(l_ref[:m, half:], b1_ref[:, at], preferred_element_type=F32)
                return base + (LORA_SCALE * delta).astype(BF16).astype(F32)

            gate = branch(wg_ref, lg_ref, bg0_ref, bg1_ref)
            up = branch(wu_ref, lu_ref, bu0_ref, bu1_ref)
            h_ref[:m, at] = (jax.nn.silu(gate) * up).astype(BF16)
            return carry

        lax.fori_loop(0, h_ref.shape[1] // sub, columns, 0)

    per_row_count(info_ref, counts, body)


def gate_up(info, x, lg, lu, wg, wu, bg0, bg1, bu0, bu1, block=512, sub=256):
    tok, d = x.shape
    f = wg.shape[1]
    low = lg.shape[1]
    counts = row_counts(tok)
    spec_w = pl.BlockSpec((d, block), lambda i, info: (0, i))
    spec_b = pl.BlockSpec((low // 2, block), lambda i, info: (0, i))
    return pl.pallas_call(
        functools.partial(up_kernel, counts, sub),
        grid_spec=pltpu.PrefetchScalarGridSpec(
            num_scalar_prefetch=1,
            grid=(f // block,),
            in_specs=[whole((tok, d)), whole((tok, low)), whole((tok, low)), spec_w, spec_w, spec_b, spec_b, spec_b, spec_b],
            out_specs=pl.BlockSpec((tok, block), lambda i, info: (0, i)),
        ),
        out_shape=jax.ShapeDtypeStruct((tok, f), BF16),
        compiler_params=pltpu.CompilerParams(vmem_limit_bytes=VMEM_LIMIT),
        cost_estimate=pl.CostEstimate(flops=4 * tok * (d + low) * f, bytes_accessed=4 * f * (d + low), transcendentals=tok * f),
    )(info, x, lg, lu, wg, wu, bg0, bg1, bu0, bu1)


def down_kernel(counts, rank, sub, info_ref, x_ref, lid_ref, h_ref, wd_ref, a0_ref, a1_ref, b0_ref, b1_ref, o_ref, acc_ref, low_ref, ld_ref):
    step = pl.program_id(0)
    tok, d = acc_ref.shape
    half = a0_ref.shape[0]

    def body(m):
        def columns(i, first):
            at = pl.ds(pl.multiple_of(i * sub, sub), sub)
            part = jnp.dot(h_ref[:m, :], wd_ref[:, at], preferred_element_type=F32)
            if first:
                acc_ref[:m, at] = part
            else:
                acc_ref[:m, at] += part

        def lows(first):
            for side, a_ref in ((0, a0_ref), (1, a1_ref)):
                at = slice(side * half, (side + 1) * half)
                part = lax.dot_general(h_ref[:m, :], a_ref[...], NT, preferred_element_type=F32)
                if first:
                    low_ref[:m, at] = part
                else:
                    low_ref[:m, at] += part

        @pl.when(step == 0)
        def _():
            acc_ref[:m, :] = jnp.zeros((m, d), F32)
            low_ref[:m, :] = jnp.zeros((m, 2 * half), F32)

        def loop(i, carry):
            columns(i, False)
            return carry

        lax.fori_loop(0, d // sub, loop, 0)
        lows(False)

        @pl.when(step == pl.num_programs(0) - 1)
        def _():
            column = lax.broadcasted_iota(jnp.int32, (m, 2 * half), 1)
            mine = (column // rank) == lid_ref[:m, :]
            ld_ref[:m, :] = jnp.where(mine, low_ref[:m, :], 0.0).astype(BF16)

            def finish(i, carry):
                at = pl.ds(pl.multiple_of(i * sub, sub), sub)
                delta = jnp.dot(ld_ref[:m, :half], b0_ref[:, at], preferred_element_type=F32)
                delta += jnp.dot(ld_ref[:m, half:], b1_ref[:, at], preferred_element_type=F32)
                down = acc_ref[:m, at] + (LORA_SCALE * delta).astype(BF16).astype(F32)
                o_ref[:m, at] = (x_ref[:m, at].astype(F32) + down).astype(BF16)
                return carry

            lax.fori_loop(0, d // sub, finish, 0)
            if m < tok:
                o_ref[m:, :] = jnp.zeros((tok - m, d), BF16)

    per_row_count(info_ref, counts, body)


def down(info, x, lid, h, wd, ad, bd0, bd1, rank, block=512, sub=512):
    tok, d = x.shape
    f = h.shape[1]
    half = bd0.shape[0]
    counts = row_counts(tok)
    return pl.pallas_call(
        functools.partial(down_kernel, counts, rank, sub),
        grid_spec=pltpu.PrefetchScalarGridSpec(
            num_scalar_prefetch=1,
            grid=(f // block,),
            in_specs=[
                whole((tok, d)),
                whole((tok, 1)),
                pl.BlockSpec((tok, block), lambda i, info: (0, i)),
                pl.BlockSpec((block, d), lambda i, info: (i, 0)),
                pl.BlockSpec((half, block), lambda i, info: (info[1], i)),
                pl.BlockSpec((half, block), lambda i, info: (info[1] ^ 1, i)),
                whole((half, d)),
                whole((half, d)),
            ],
            out_specs=pl.BlockSpec((tok, d), lambda i, info: (0, 0)),
            scratch_shapes=[pltpu.VMEM((tok, d), F32), pltpu.VMEM((tok, 2 * half), F32), pltpu.VMEM((tok, 2 * half), BF16)],
        ),
        out_shape=jax.ShapeDtypeStruct((tok, d), BF16),
        compiler_params=pltpu.CompilerParams(vmem_limit_bytes=VMEM_LIMIT),
        cost_estimate=pl.CostEstimate(flops=2 * tok * (d + 2 * half) * f, bytes_accessed=2 * f * (d + 2 * half + tok), transcendentals=0),
    )(info, x, lid, h, wd, ad, ad, bd0, bd1)


def solution(mesh):
    groups = mesh.shape['data']
    assert groups == 4
    row_spec = P(('rep', 'data'), None)
    tok_spec = P(('rep', 'data'))
    full_two = P(None, None)
    full_three = P(None, None, None)
    owned = P('data', None, None)
    to_chip = [(j, j ^ 2) for j in range(groups)]
    to_core = [(j, j ^ 1) for j in range(groups)]

    def device_fn(hidden, adapter_id, w_gate, w_up, w_down, a_gate, b_gate, a_up, b_up, a_down, b_down):
        tok, d = hidden.shape
        adapters, f, rank = a_down.shape
        per_owner = b_gate.shape[0]
        own_rows = per_owner * rank
        me = lax.axis_index('data').astype(jnp.int32)

        bg0, bu0, bd0 = (b.reshape(own_rows, b.shape[2]) for b in (b_gate, b_up, b_down))
        bg1, bu1, bd1 = (lax.ppermute(b, 'data', to_core) for b in (bg0, bu0, bd0))
        ag, au, ad = (jnp.transpose(a, (0, 2, 1)).reshape(adapters * rank, a.shape[1]) for a in (a_gate, a_up, a_down))

        owner = adapter_id // per_owner
        cross = (owner // 2) != (me // 2)
        lid = ((owner ^ me) & 1) * per_owner + adapter_id % per_owner
        token = jnp.arange(tok, dtype=jnp.int32)
        before = token[None, :] < token[:, None]

        def place(chosen):
            rank_of = jnp.sum((before & chosen[None, :]).astype(jnp.int32), axis=1)
            hot = (token[:, None] == rank_of[None, :]) & chosen[None, :]
            rows = jnp.dot(hot.astype(BF16), hidden, preferred_element_type=F32).astype(BF16)
            lids = jnp.sum(hot.astype(jnp.int32) * (lid[None, :] + 1), axis=1) - 1
            return hot.astype(BF16), rows, lids

        cross_hot, send_x, send_lid = place(cross)
        recv_x = lax.ppermute(send_x, 'data', to_chip)
        recv_lid = lax.ppermute(send_lid, 'data', to_chip)
        stay_hot, stay_x, stay_lid = place(~cross)

        def hidden_rows(x, lids):
            info = jnp.stack([jnp.sum((lids >= 0).astype(jnp.int32)), me])
            lg, lu = low_rows(info, x, lids[:, None], ag, au, own_rows, rank)
            return info, gate_up(info, x, lg, lu, w_gate, w_up, bg0, bg1, bu0, bu1)

        stay_info, stay_h = hidden_rows(stay_x, stay_lid)
        recv_info, recv_h = hidden_rows(recv_x, recv_lid)
        recv_y = down(recv_info, recv_x, recv_lid[:, None], recv_h, w_down, ad, bd0, bd1, rank)
        back_y = lax.ppermute(recv_y, 'data', to_chip)
        stay_y = down(stay_info, stay_x, stay_lid[:, None], stay_h, w_down, ad, bd0, bd1, rank)

        pick = (((0,), (0,)), ((), ()))
        out = lax.dot_general(stay_hot, stay_y, pick, preferred_element_type=F32)
        out += lax.dot_general(cross_hot, back_y, pick, preferred_element_type=F32)
        return out.astype(BF16)

    return jax.shard_map(device_fn, mesh=mesh, in_specs=(row_spec, tok_spec, full_two, full_two, full_two, full_three, owned, full_three, owned, full_three, owned), out_specs=row_spec, check_vma=False)
```

```python
import functools

import jax
import jax.numpy as jnp
from jax import lax
from jax.experimental import pallas as pl
from jax.experimental.pallas import tpu as pltpu
from jax.sharding import PartitionSpec as P

LORA_SCALE = 2.0
F32 = jnp.float32
BF16 = jnp.bfloat16
NT = (((1,), (1,)), ((), ()))
VMEM_LIMIT = 62 * 1024 * 1024


def row_counts(tok):
    if tok == 512:
        return (256, 352, 368, 512)
    return (tok // 2, tok)


def per_row_count(rows_ref, counts, body):
    rows = rows_ref[0]
    below = 0
    for count in counts:
        pl.when((rows > below) & (rows <= count))(functools.partial(body, count))
        below = count


def whole(shape):
    zeros = (0,) * len(shape)
    return pl.BlockSpec(shape, lambda *_: zeros, pipeline_mode=pl.Buffered(1))


def low_kernel(counts, rank, info_ref, x_ref, lid_ref, ag_ref, au_ref, lg_ref, lu_ref):
    width = ag_ref.shape[0]
    block = pl.program_id(0)

    def body(m):
        column = block * width + lax.broadcasted_iota(jnp.int32, (m, width), 1)
        mine = (column // rank) == lid_ref[:m, :]
        for a_ref, l_ref in ((ag_ref, lg_ref), (au_ref, lu_ref)):
            low = lax.dot_general(x_ref[:m, :], a_ref[...], NT, preferred_element_type=F32)
            l_ref[:m, :] = jnp.where(mine, low, 0.0).astype(BF16)

    per_row_count(info_ref, counts, body)


def low_rows(info, x, lid, ag, au, own_rows, rank):
    tok, d = x.shape
    width = own_rows // 2
    counts = row_counts(tok)
    spec_a = pl.BlockSpec((width, d), lambda b, info: ((info[1] ^ (b // 2)) * 2 + b % 2, 0))
    spec_l = pl.BlockSpec((tok, width), lambda b, info: (0, b))
    return pl.pallas_call(
        functools.partial(low_kernel, counts, rank),
        grid_spec=pltpu.PrefetchScalarGridSpec(
            num_scalar_prefetch=1,
            grid=(4,),
            in_specs=[whole((tok, d)), whole((tok, 1)), spec_a, spec_a],
            out_specs=[spec_l, spec_l],
        ),
        out_shape=[jax.ShapeDtypeStruct((tok, 4 * width), BF16)] * 2,
        compiler_params=pltpu.CompilerParams(vmem_limit_bytes=VMEM_LIMIT),
        cost_estimate=pl.CostEstimate(flops=2 * 2 * tok * d * 4 * width, bytes_accessed=4 * 4 * width * d, transcendentals=0),
    )(info, x, lid, ag, au)


def mlp_kernel(counts, rank, sub, wide, info_ref, x_ref, lid_ref, lg_ref, lu_ref, wg_ref, wu_ref, bg0_ref, bg1_ref, bu0_ref, bu1_ref,
               wd_ref, a0_ref, a1_ref, bd0_ref, bd1_ref, o_ref, acc_ref, low_ref, ld_ref):
    step = pl.program_id(0)
    tok, d = acc_ref.shape
    half = bg0_ref.shape[0]
    block = wg_ref.shape[1]

    def body(m):
        def branch(at, w_ref, l_ref, b0_ref, b1_ref):
            base = jnp.dot(x_ref[:m, :], w_ref[:, at], preferred_element_type=F32)
            delta = jnp.dot(l_ref[:m, :half], b0_ref[:, at], preferred_element_type=F32)
            delta += jnp.dot(l_ref[:m, half:], b1_ref[:, at], preferred_element_type=F32)
            return base + (LORA_SCALE * delta).astype(BF16).astype(F32)

        @pl.when(step == 0)
        def _():
            acc_ref[:m, :] = jnp.zeros((m, d), F32)
            low_ref[:m, :] = jnp.zeros((m, 2 * half), F32)

        for first in range(0, block, sub):
            at = slice(first, first + sub)
            gate = branch(at, wg_ref, lg_ref, bg0_ref, bg1_ref)
            up = branch(at, wu_ref, lu_ref, bu0_ref, bu1_ref)
            h = (jax.nn.silu(gate) * up).astype(BF16)
            for left in range(0, d, wide):
                to = slice(left, left + wide)
                acc_ref[:m, to] += jnp.dot(h, wd_ref[at, to], preferred_element_type=F32)
            for side, a_ref in ((0, a0_ref), (1, a1_ref)):
                to = slice(side * half, (side + 1) * half)
                low_ref[:m, to] += lax.dot_general(h, a_ref[:, at], NT, preferred_element_type=F32)

        @pl.when(step == pl.num_programs(0) - 1)
        def _():
            column = lax.broadcasted_iota(jnp.int32, (m, 2 * half), 1)
            mine = (column // rank) == lid_ref[:m, :]
            ld_ref[:m, :] = jnp.where(mine, low_ref[:m, :], 0.0).astype(BF16)

            def finish(i, carry):
                to = pl.ds(pl.multiple_of(i * wide, wide), wide)
                delta = jnp.dot(ld_ref[:m, :half], bd0_ref[:, to], preferred_element_type=F32)
                delta += jnp.dot(ld_ref[:m, half:], bd1_ref[:, to], preferred_element_type=F32)
                down = acc_ref[:m, to] + (LORA_SCALE * delta).astype(BF16).astype(F32)
                o_ref[:m, to] = (x_ref[:m, to].astype(F32) + down).astype(BF16)
                return carry

            lax.fori_loop(0, d // wide, finish, 0)
            if m < tok:
                o_ref[m:, :] = jnp.zeros((tok - m, d), BF16)

    per_row_count(info_ref, counts, body)


def mlp(info, x, lid, lg, lu, wg, wu, bg0, bg1, bu0, bu1, wd, ad, bd0, bd1, rank, block=512, sub=256, wide=512):
    tok, d = x.shape
    f = wg.shape[1]
    low = lg.shape[1]
    half = low // 2
    counts = row_counts(tok)
    spec_w = pl.BlockSpec((d, block), lambda i, info: (0, i))
    spec_b = pl.BlockSpec((half, block), lambda i, info: (0, i))
    return pl.pallas_call(
        functools.partial(mlp_kernel, counts, rank, sub, wide),
        grid_spec=pltpu.PrefetchScalarGridSpec(
            num_scalar_prefetch=1,
            grid=(f // block,),
            in_specs=[
                whole((tok, d)), whole((tok, 1)), whole((tok, low)), whole((tok, low)),
                spec_w, spec_w, spec_b, spec_b, spec_b, spec_b,
                pl.BlockSpec((block, d), lambda i, info: (i, 0)),
                pl.BlockSpec((half, block), lambda i, info: (info[1], i)),
                pl.BlockSpec((half, block), lambda i, info: (info[1] ^ 1, i)),
                whole((half, d)), whole((half, d)),
            ],
            out_specs=whole((tok, d)),
            scratch_shapes=[pltpu.VMEM((tok, d), F32), pltpu.VMEM((tok, low), F32), pltpu.VMEM((tok, low), BF16)],
        ),
        out_shape=jax.ShapeDtypeStruct((tok, d), BF16),
        compiler_params=pltpu.CompilerParams(vmem_limit_bytes=VMEM_LIMIT),
        cost_estimate=pl.CostEstimate(flops=6 * tok * (d + low) * f, bytes_accessed=6 * f * (d + low), transcendentals=tok * f),
    )(info, x, lid, lg, lu, wg, wu, bg0, bg1, bu0, bu1, wd, ad, ad, bd0, bd1)


def solution(mesh):
    groups = mesh.shape['data']
    assert groups == 4
    row_spec = P(('rep', 'data'), None)
    tok_spec = P(('rep', 'data'))
    full_two = P(None, None)
    full_three = P(None, None, None)
    owned = P('data', None, None)
    to_chip = [(j, j ^ 2) for j in range(groups)]
    to_core = [(j, j ^ 1) for j in range(groups)]

    def device_fn(hidden, adapter_id, w_gate, w_up, w_down, a_gate, b_gate, a_up, b_up, a_down, b_down):
        tok, d = hidden.shape
        adapters, f, rank = a_down.shape
        per_owner = b_gate.shape[0]
        own_rows = per_owner * rank
        me = lax.axis_index('data').astype(jnp.int32)

        bg0, bu0, bd0 = (b.reshape(own_rows, b.shape[2]) for b in (b_gate, b_up, b_down))
        bg1, bu1, bd1 = (lax.ppermute(b, 'data', to_core) for b in (bg0, bu0, bd0))
        ag, au, ad = (jnp.transpose(a, (0, 2, 1)).reshape(adapters * rank, a.shape[1]) for a in (a_gate, a_up, a_down))

        owner = adapter_id // per_owner
        cross = (owner // 2) != (me // 2)
        lid = ((owner ^ me) & 1) * per_owner + adapter_id % per_owner
        token = jnp.arange(tok, dtype=jnp.int32)
        before = token[None, :] < token[:, None]

        def place(chosen):
            rank_of = jnp.sum((before & chosen[None, :]).astype(jnp.int32), axis=1)
            hot = (token[:, None] == rank_of[None, :]) & chosen[None, :]
            rows = jnp.dot(hot.astype(BF16), hidden, preferred_element_type=F32).astype(BF16)
            lids = jnp.sum(hot.astype(jnp.int32) * (lid[None, :] + 1), axis=1) - 1
            return hot.astype(BF16), rows, lids

        cross_hot, send_x, send_lid = place(cross)
        recv_x = lax.ppermute(send_x, 'data', to_chip)
        recv_lid = lax.ppermute(send_lid, 'data', to_chip)
        stay_hot, stay_x, stay_lid = place(~cross)

        def out_rows(x, lids):
            info = jnp.stack([jnp.sum((lids >= 0).astype(jnp.int32)), me])
            lid_rows = lids[:, None]
            lg, lu = low_rows(info, x, lid_rows, ag, au, own_rows, rank)
            return mlp(info, x, lid_rows, lg, lu, w_gate, w_up, bg0, bg1, bu0, bu1, w_down, ad, bd0, bd1, rank)

        recv_y = out_rows(recv_x, recv_lid)
        back_y = lax.ppermute(recv_y, 'data', to_chip)
        stay_y = out_rows(stay_x, stay_lid)

        pick = (((0,), (0,)), ((), ()))
        out = lax.dot_general(stay_hot, stay_y, pick, preferred_element_type=F32)
        out += lax.dot_general(cross_hot, back_y, pick, preferred_element_type=F32)
        return out.astype(BF16)

    return jax.shard_map(device_fn, mesh=mesh, in_specs=(row_spec, tok_spec, full_two, full_two, full_two, full_three, owned, full_three, owned, full_three, owned), out_specs=row_spec, check_vma=False)
```

```python
import functools

import jax
import jax.numpy as jnp
from jax import lax
from jax.experimental import pallas as pl
from jax.experimental.pallas import tpu as pltpu
from jax.sharding import PartitionSpec as P


LORA_SCALE = 2.0
F32 = jnp.float32
BF16 = jnp.bfloat16
NT = (((1,), (1,)), ((), ()))
VMEM_LIMIT = 62 * 1024 * 1024
BLOCK = 512


def row_counts(tok):
    if tok == 512:
        return (352, 368, 512)
    return (tok // 2, tok)


def per_row_count(rows_ref, counts, body):
    rows = rows_ref[0]
    below = 0
    for count in counts:
        pl.when((rows > below) & (rows <= count))(functools.partial(body, count))
        below = count


def whole(shape):
    zeros = (0,) * len(shape)
    return pl.BlockSpec(shape, lambda *_: zeros, pipeline_mode=pl.Buffered(1))


def low_kernel(counts, rank, info_ref, x_ref, lid_ref, ag_ref, au_ref, lg_ref, lu_ref):
    width = ag_ref.shape[0]
    block = pl.program_id(0)

    def body(m):
        column = block * width + lax.broadcasted_iota(jnp.int32, (m, width), 1)
        mine = (column // rank) == lid_ref[:m, :]
        for a_ref, l_ref in ((ag_ref, lg_ref), (au_ref, lu_ref)):
            low = lax.dot_general(x_ref[:m, :], a_ref[...], NT, preferred_element_type=F32)
            l_ref[:m, :] = jnp.where(mine, low, 0.0).astype(BF16)

    per_row_count(info_ref, counts, body)


def low_rows(info, x, lid, ag, au, own_rows, rank):
    tok, d = x.shape
    width = own_rows // 2
    counts = row_counts(tok)
    spec_a = pl.BlockSpec((width, d), lambda b, info: ((info[1] ^ (b // 2)) * 2 + b % 2, 0))
    spec_l = pl.BlockSpec((tok, width), lambda b, info: (0, b))
    return pl.pallas_call(
        functools.partial(low_kernel, counts, rank),
        grid_spec=pltpu.PrefetchScalarGridSpec(
            num_scalar_prefetch=1,
            grid=(4,),
            in_specs=[whole((tok, d)), whole((tok, 1)), spec_a, spec_a],
            out_specs=[spec_l, spec_l],
        ),
        out_shape=[jax.ShapeDtypeStruct((tok, 4 * width), BF16)] * 2,
        compiler_params=pltpu.CompilerParams(vmem_limit_bytes=VMEM_LIMIT),
        cost_estimate=pl.CostEstimate(flops=2 * 2 * tok * d * 4 * width, bytes_accessed=4 * 4 * width * d, transcendentals=0),
    )(info, x, lid, ag, au)


def mlp_kernel(counts, rank, sub, wide, resume, final, info_ref, x_ref, lid_ref, lg_ref, lu_ref, wg_ref, wu_ref, bg0_ref, bg1_ref,
               bu0_ref, bu1_ref, wd_ref, a0_ref, a1_ref, *refs):
    refs = list(refs)
    bd0_ref, bd1_ref = (refs.pop(0), refs.pop(0)) if final else (None, None)
    acc_in, low_in = (refs.pop(0), refs.pop(0)) if resume else (None, None)
    o_ref = refs.pop(0) if final else None
    acc_out, low_out = (None, None) if final else (refs.pop(0), refs.pop(0))
    acc_ref, low_ref, ld_ref, sems = refs
    step = pl.program_id(0)
    tok, d = acc_ref.shape
    half = bg0_ref.shape[0]
    block = wg_ref.shape[1]

    def move(pairs):
        copies = [pltpu.make_async_copy(src, dst, sems.at[i]) for i, (src, dst) in enumerate(pairs)]
        for copy in copies:
            copy.start()
        for copy in copies:
            copy.wait()

    def body(m):
        def branch(at, w_ref, l_ref, b0_ref, b1_ref):
            base = jnp.dot(x_ref[:m, :], w_ref[:, at], preferred_element_type=F32)
            delta = jnp.dot(l_ref[:m, :half], b0_ref[:, at], preferred_element_type=F32)
            delta += jnp.dot(l_ref[:m, half:], b1_ref[:, at], preferred_element_type=F32)
            return base + (LORA_SCALE * delta).astype(BF16).astype(F32)

        @pl.when(step == 0)
        def _():
            if resume:
                move(((acc_in, acc_ref), (low_in, low_ref)))
            else:
                acc_ref[:m, :] = jnp.zeros((m, d), F32)
                low_ref[:m, :] = jnp.zeros((m, 2 * half), F32)

        def gate_up(at):
            return at, branch(at, wg_ref, lg_ref, bg0_ref, bg1_ref), branch(at, wu_ref, lu_ref, bu0_ref, bu1_ref)

        def add_down(at, gate, up):
            h = (jax.nn.silu(gate) * up).astype(BF16)
            for left in range(0, d, wide):
                to = slice(left, left + wide)
                acc_ref[:m, to] += jnp.dot(h, wd_ref[at, to], preferred_element_type=F32)
            for side, a_ref in ((0, a0_ref), (1, a1_ref)):
                to = slice(side * half, (side + 1) * half)
                low_ref[:m, to] += lax.dot_general(h, a_ref[:, at], NT, preferred_element_type=F32)

        waiting = None
        for first in range(0, block, sub):
            now = gate_up(slice(first, first + sub))
            if waiting is not None:
                add_down(*waiting)
            waiting = now
        add_down(*waiting)

        @pl.when(step == pl.num_programs(0) - 1)
        def _():
            if not final:
                move(((acc_ref, acc_out), (low_ref, low_out)))
                return
            column = lax.broadcasted_iota(jnp.int32, (m, 2 * half), 1)
            mine = (column // rank) == lid_ref[:m, :]
            ld_ref[:m, :] = jnp.where(mine, low_ref[:m, :], 0.0).astype(BF16)

            def finish(i, carry):
                to = pl.ds(pl.multiple_of(i * wide, wide), wide)
                delta = jnp.dot(ld_ref[:m, :half], bd0_ref[:, to], preferred_element_type=F32)
                delta += jnp.dot(ld_ref[:m, half:], bd1_ref[:, to], preferred_element_type=F32)
                down = acc_ref[:m, to] + (LORA_SCALE * delta).astype(BF16).astype(F32)
                o_ref[:m, to] = (x_ref[:m, to].astype(F32) + down).astype(BF16)
                return carry

            lax.fori_loop(0, d // wide, finish, 0)
            if m < tok:
                o_ref[m:, :] = jnp.zeros((tok - m, d), BF16)

    per_row_count(info_ref, counts, body)


def mlp(info, x, lid, lg, lu, wg, wu, bs, wd, ad, bd, rank, first, stop, sums=None, block=BLOCK, sub=256, wide=512):
    tok, d = x.shape
    low = lg.shape[1]
    half = low // 2
    counts = row_counts(tok)
    resume, final = sums is not None, bd is not None
    spec_w = pl.BlockSpec((d, block), lambda i, info: (0, i + first))
    any_spec = pl.BlockSpec(memory_space=pl.ANY)
    in_specs = [
        whole((tok, d)), whole((tok, 1)), whole((tok, low)), whole((tok, low)), spec_w, spec_w,
        *(pl.BlockSpec((half, block), lambda i, info, off=0 if local else first: (0, i + off)) for _, local in bs),
        pl.BlockSpec((block, d), lambda i, info: (i + first, 0)),
        pl.BlockSpec((half, block), lambda i, info: (info[1], i + first)),
        pl.BlockSpec((half, block), lambda i, info: (info[1] ^ 1, i + first)),
    ]
    args = [x, lid, lg, lu, wg, wu, *(b for b, _ in bs), wd, ad, ad]
    if final:
        in_specs += [whole((half, d))] * 2
        args += bd
        out_specs, out_shape = whole((tok, d)), jax.ShapeDtypeStruct((tok, d), BF16)
    else:
        out_specs = [any_spec] * 2
        out_shape = [jax.ShapeDtypeStruct((tok, d), F32), jax.ShapeDtypeStruct((tok, low), F32)]
    if resume:
        in_specs += [any_spec] * 2
        args += sums
    width = (stop - first) * block
    return pl.pallas_call(
        functools.partial(mlp_kernel, counts, rank, sub, wide, resume, final),
        grid_spec=pltpu.PrefetchScalarGridSpec(
            num_scalar_prefetch=1,
            grid=(stop - first,),
            in_specs=in_specs,
            out_specs=out_specs,
            scratch_shapes=[pltpu.VMEM((tok, d), F32), pltpu.VMEM((tok, low), F32), pltpu.VMEM((tok, low), BF16), pltpu.SemaphoreType.DMA((2,))],
        ),
        out_shape=out_shape,
        compiler_params=pltpu.CompilerParams(vmem_limit_bytes=VMEM_LIMIT),
        cost_estimate=pl.CostEstimate(flops=6 * tok * (d + low) * width if final else 1000, bytes_accessed=6 * width * (d + low), transcendentals=tok * width),
    )(info, *args)


def solution(mesh):
    groups = mesh.shape['data']
    assert groups == 4
    row_spec = P(('rep', 'data'), None)
    tok_spec = P(('rep', 'data'))
    full_two = P(None, None)
    full_three = P(None, None, None)
    owned = P('data', None, None)
    to_chip = [(j, j ^ 2) for j in range(groups)]
    to_core = [(j, j ^ 1) for j in range(groups)]

    def device_fn(hidden, adapter_id, w_gate, w_up, w_down, a_gate, b_gate, a_up, b_up, a_down, b_down):
        tok, _ = hidden.shape
        adapters, f, rank = a_down.shape
        per_owner = b_gate.shape[0]
        own_rows = per_owner * rank
        me = lax.axis_index('data').astype(jnp.int32)

        blocks = f // BLOCK
        early = max(1, blocks // 3)

        bg0, bu0, bd0 = (b.reshape(own_rows, b.shape[2]) for b in (b_gate, b_up, b_down))
        bg1_early, bu1_early = (lax.ppermute(b[:, :early * BLOCK], 'data', to_core) for b in (bg0, bu0))
        ag, au, ad = (jnp.transpose(a, (0, 2, 1)).reshape(adapters * rank, a.shape[1]) for a in (a_gate, a_up, a_down))

        owner = adapter_id // per_owner
        cross = (owner // 2) != (me // 2)
        lid = ((owner ^ me) & 1) * per_owner + adapter_id % per_owner
        token = jnp.arange(tok, dtype=jnp.int32)
        before = token[None, :] < token[:, None]

        def place(chosen, hidden):
            rank_of = jnp.sum((before & chosen[None, :]).astype(jnp.int32), axis=1)
            hot = (token[:, None] == rank_of[None, :]) & chosen[None, :]
            rows = jnp.dot(hot.astype(BF16), hidden, preferred_element_type=F32).astype(BF16)
            lids = jnp.sum(hot.astype(jnp.int32) * (lid[None, :] + 1), axis=1) - 1
            return hot.astype(BF16), rows, lids

        cross_hot, send_x, send_lid = place(cross, hidden)
        send_x, rows = lax.optimization_barrier((send_x, hidden))
        recv_x = lax.ppermute(send_x, 'data', to_chip)
        recv_lid = lax.ppermute(send_lid, 'data', to_chip)
        stay_hot, stay_x, stay_lid = place(~cross, rows)

        def low(x, lids):
            info = jnp.stack([jnp.sum((lids >= 0).astype(jnp.int32)), me])
            lid_rows = lids[:, None]
            lg, lu = low_rows(info, x, lid_rows, ag, au, own_rows, rank)
            return info, x, lid_rows, lg, lu, w_gate, w_up

        stay = low(stay_x, stay_lid)
        late = lax.optimization_barrier((bg0, bu0, bd0, bg1_early, bu1_early, stay))
        bg1, bu1, bd1 = (lax.ppermute(b, 'data', to_core) for b in late[:3])
        bg1_early, bu1_early, stay = late[3:]
        b_all = [(bg0, False), (bg1, False), (bu0, False), (bu1, False)]
        b_early = [(bg0, False), (bg1_early, True), (bu0, False), (bu1_early, True)]
        b_out = [bd0, bd1]
        sums = mlp(*stay, b_early, w_down, ad, None, rank, 0, early)
        recv_x, recv_lid, sums = lax.optimization_barrier((recv_x, recv_lid, sums))
        recv_y = mlp(*low(recv_x, recv_lid), b_all, w_down, ad, b_out, rank, 0, blocks)
        back_y = lax.ppermute(recv_y, 'data', to_chip)
        recv_y, sums = lax.optimization_barrier((recv_y, sums))
        stay_y = mlp(*stay, b_all, w_down, ad, b_out, rank, early, blocks, sums)

        pick = (((0,), (0,)), ((), ()))
        out = lax.dot_general(stay_hot, stay_y, pick, preferred_element_type=F32)
        out += lax.dot_general(cross_hot, back_y, pick, preferred_element_type=F32)
        return out.astype(BF16)

    return jax.shard_map(device_fn, mesh=mesh, in_specs=(row_spec, tok_spec, full_two, full_two, full_two, full_three, owned, full_three, owned, full_three, owned), out_specs=row_spec, check_vma=False)
```

```python
import functools

import jax
import jax.numpy as jnp
from jax import lax
from jax.experimental import pallas as pl
from jax.experimental.pallas import tpu as pltpu
from jax.sharding import PartitionSpec as P


LORA_SCALE = 2.0
F32 = jnp.float32
BF16 = jnp.bfloat16
NT = (((1,), (1,)), ((), ()))
VMEM_LIMIT = 62 * 1024 * 1024
BLOCK = 512


def row_cases(tok):
    if tok == 512:
        return ((256, 352), (96, 352), (256, 368), (112, 368), (256, 512))
    return ((tok // 2, tok),)


def per_case(info_ref, tok, body):
    for index, (split, rows) in enumerate(row_cases(tok)):
        pl.when(info_ref[0] == index)(functools.partial(body, split, rows))


def whole(shape):
    zeros = (0,) * len(shape)
    return pl.BlockSpec(shape, lambda *_: zeros, pipeline_mode=pl.Buffered(1))


def low_kernel(rank, info_ref, x_ref, lid_ref, ag0_ref, ag1_ref, au0_ref, au1_ref, lg_ref, lu_ref):
    width = ag0_ref.shape[0]
    block = pl.program_id(0)

    def body(split, m):
        def masked(rows, a_ref):
            low = lax.dot_general(x_ref[rows, :], a_ref[...], NT, preferred_element_type=F32)
            column = block * width + lax.broadcasted_iota(jnp.int32, low.shape, 1)
            return jnp.where((column // rank) == lid_ref[rows, :], low, 0.0).astype(BF16)

        for a0_ref, a1_ref, l_ref in ((ag0_ref, ag1_ref, lg_ref), (au0_ref, au1_ref, lu_ref)):
            l_ref[:split, :] = masked(slice(0, split), a0_ref)
            l_ref[split:m, :] = masked(slice(split, m), a1_ref)

    per_case(info_ref, x_ref.shape[0], body)


def low_rows(info, x, lid, ag, au, own_rows, rank):
    tok, d = x.shape
    width = own_rows // 2
    spec_a = [pl.BlockSpec((width, d), lambda b, info, side=side: ((info[1] ^ side) * 2 + b, 0)) for side in (0, 1)]
    spec_l = pl.BlockSpec((tok, width), lambda b, info: (0, b))
    return pl.pallas_call(
        functools.partial(low_kernel, rank),
        grid_spec=pltpu.PrefetchScalarGridSpec(
            num_scalar_prefetch=1,
            grid=(2,),
            in_specs=[whole((tok, d)), whole((tok, 1)), *spec_a, *spec_a],
            out_specs=[spec_l, spec_l],
        ),
        out_shape=[jax.ShapeDtypeStruct((tok, own_rows), BF16)] * 2,
        compiler_params=pltpu.CompilerParams(vmem_limit_bytes=VMEM_LIMIT),
        cost_estimate=pl.CostEstimate(flops=4 * tok * d * own_rows, bytes_accessed=8 * own_rows * d, transcendentals=0),
    )(info, x, lid, ag, ag, au, au)


def mlp_kernel(rank, sub, wide, resume, final, info_ref, x_ref, lid_ref, lg_ref, lu_ref, wg_ref, wu_ref, bg0_ref, bg1_ref,
               bu0_ref, bu1_ref, wd_ref, a0_ref, a1_ref, *refs):
    refs = list(refs)
    bd0_ref, bd1_ref = (refs.pop(0), refs.pop(0)) if final else (None, None)
    acc_in, low_in = (refs.pop(0), refs.pop(0)) if resume else (None, None)
    o_ref = refs.pop(0) if final else None
    acc_out, low_out = (None, None) if final else (refs.pop(0), refs.pop(0))
    acc_ref, low_ref, ld_ref, sems = refs
    step = pl.program_id(0)
    tok, d = acc_ref.shape
    half = bg0_ref.shape[0]
    block = wg_ref.shape[1]

    def move(pairs):
        copies = [pltpu.make_async_copy(src, dst, sems.at[i]) for i, (src, dst) in enumerate(pairs)]
        for copy in copies:
            copy.start()
        for copy in copies:
            copy.wait()

    def body(split, m):
        def spread(l_ref, at, b0_ref, b1_ref):
            own = jnp.dot(l_ref[:split, :], b0_ref[:, at], preferred_element_type=F32)
            partner = jnp.dot(l_ref[split:m, :], b1_ref[:, at], preferred_element_type=F32)
            return (LORA_SCALE * jnp.concatenate([own, partner], axis=0)).astype(BF16).astype(F32)

        def branch(at, w_ref, l_ref, b0_ref, b1_ref):
            base = jnp.dot(x_ref[:m, :], w_ref[:, at], preferred_element_type=F32)
            return base + spread(l_ref, at, b0_ref, b1_ref)

        @pl.when(step == 0)
        def _():
            if resume:
                move(((acc_in, acc_ref), (low_in, low_ref)))
            else:
                acc_ref[:m, :] = jnp.zeros((m, d), F32)
                low_ref[:m, :] = jnp.zeros((m, half), F32)

        def gate_up(at):
            return at, branch(at, wg_ref, lg_ref, bg0_ref, bg1_ref), branch(at, wu_ref, lu_ref, bu0_ref, bu1_ref)

        def add_down(at, gate, up):
            h = (jax.nn.silu(gate) * up).astype(BF16)
            for rows, a_ref in ((slice(0, split), a0_ref), (slice(split, m), a1_ref)):
                low_ref[rows, :] += lax.dot_general(h[rows, :], a_ref[:, at], NT, preferred_element_type=F32)
            for left in range(0, d, wide):
                to = slice(left, left + wide)
                acc_ref[:m, to] += jnp.dot(h, wd_ref[at, to], preferred_element_type=F32)

        waiting = None
        for first in range(0, block, sub):
            now = gate_up(slice(first, first + sub))
            if waiting is not None:
                add_down(*waiting)
            waiting = now
        add_down(*waiting)

        @pl.when(step == pl.num_programs(0) - 1)
        def _():
            if not final:
                move(((acc_ref, acc_out), (low_ref, low_out)))
                return
            column = lax.broadcasted_iota(jnp.int32, (m, half), 1)
            mine = (column // rank) == lid_ref[:m, :]
            ld_ref[:m, :] = jnp.where(mine, low_ref[:m, :], 0.0).astype(BF16)

            def finish(i, carry):
                to = pl.ds(pl.multiple_of(i * wide, wide), wide)
                down = acc_ref[:m, to] + spread(ld_ref, to, bd0_ref, bd1_ref)
                o_ref[:m, to] = (x_ref[:m, to].astype(F32) + down).astype(BF16)
                return carry

            lax.fori_loop(0, d // wide, finish, 0)
            if m < tok:
                o_ref[m:, :] = jnp.zeros((tok - m, d), BF16)

    per_case(info_ref, tok, body)


def mlp(info, x, lid, lg, lu, wg, wu, bs, wd, ad, bd, rank, first, stop, sums=None, block=BLOCK, sub=256, wide=512):
    tok, d = x.shape
    low = half = lg.shape[1]
    resume, final = sums is not None, bd is not None
    spec_w = pl.BlockSpec((d, block), lambda i, info: (0, i + first))
    any_spec = pl.BlockSpec(memory_space=pl.ANY)
    in_specs = [
        whole((tok, d)), whole((tok, 1)), whole((tok, low)), whole((tok, low)), spec_w, spec_w,
        *(pl.BlockSpec((half, block), lambda i, info, off=0 if local else first: (0, i + off)) for _, local in bs),
        pl.BlockSpec((block, d), lambda i, info: (i + first, 0)),
        pl.BlockSpec((half, block), lambda i, info: (info[1], i + first)),
        pl.BlockSpec((half, block), lambda i, info: (info[1] ^ 1, i + first)),
    ]
    args = [x, lid, lg, lu, wg, wu, *(b for b, _ in bs), wd, ad, ad]
    if final:
        in_specs += [whole((half, d))] * 2
        args += bd
        out_specs, out_shape = whole((tok, d)), jax.ShapeDtypeStruct((tok, d), BF16)
    else:
        out_specs = [any_spec] * 2
        out_shape = [jax.ShapeDtypeStruct((tok, d), F32), jax.ShapeDtypeStruct((tok, low), F32)]
    if resume:
        in_specs += [any_spec] * 2
        args += sums
    width = (stop - first) * block
    return pl.pallas_call(
        functools.partial(mlp_kernel, rank, sub, wide, resume, final),
        grid_spec=pltpu.PrefetchScalarGridSpec(
            num_scalar_prefetch=1,
            grid=(stop - first,),
            in_specs=in_specs,
            out_specs=out_specs,
            scratch_shapes=[pltpu.VMEM((tok, d), F32), pltpu.VMEM((tok, low), F32), pltpu.VMEM((tok, low), BF16), pltpu.SemaphoreType.DMA((2,))],
        ),
        out_shape=out_shape,
        compiler_params=pltpu.CompilerParams(vmem_limit_bytes=VMEM_LIMIT),
        cost_estimate=pl.CostEstimate(flops=6 * tok * (d + low) * width if final else 1000, bytes_accessed=6 * width * (d + low), transcendentals=tok * width),
    )(info, *args)


def solution(mesh):
    groups = mesh.shape['data']
    assert groups == 4
    row_spec = P(('rep', 'data'), None)
    tok_spec = P(('rep', 'data'))
    full_two = P(None, None)
    full_three = P(None, None, None)
    owned = P('data', None, None)
    to_chip = [(j, j ^ 2) for j in range(groups)]
    to_core = [(j, j ^ 1) for j in range(groups)]

    def device_fn(hidden, adapter_id, w_gate, w_up, w_down, a_gate, b_gate, a_up, b_up, a_down, b_down):
        tok, _ = hidden.shape
        adapters, f, rank = a_down.shape
        per_owner = b_gate.shape[0]
        own_rows = per_owner * rank
        me = lax.axis_index('data').astype(jnp.int32)

        blocks = f // BLOCK
        early = max(1, blocks // 4)

        bg0, bu0, bd0 = (b.reshape(own_rows, b.shape[2]) for b in (b_gate, b_up, b_down))
        ag, au, ad = (jnp.transpose(a, (0, 2, 1)).reshape(adapters * rank, a.shape[1]) for a in (a_gate, a_up, a_down))

        owner = adapter_id // per_owner
        cross = (owner // 2) != (me // 2)
        partner = ((owner ^ me) & 1) == 1
        lid = adapter_id % per_owner
        token = jnp.arange(tok, dtype=jnp.int32)
        before = token[None, :] < token[:, None]
        splits, sizes = (jnp.array(column, jnp.int32) for column in zip(*row_cases(tok)))

        def place(chosen, hidden):
            own = jnp.sum((chosen & ~partner).astype(jnp.int32))
            other = jnp.sum((chosen & partner).astype(jnp.int32))
            case = jnp.argmax((own <= splits) & (other <= sizes - splits)).astype(jnp.int32)
            alike = before & chosen[None, :] & (partner[None, :] == partner[:, None])
            rank_of = jnp.sum(alike.astype(jnp.int32), axis=1) + jnp.where(partner, splits[case], 0)
            hot = (token[:, None] == rank_of[None, :]) & chosen[None, :]
            rows = jnp.dot(hot.astype(BF16), hidden, preferred_element_type=F32).astype(BF16)
            lids = jnp.sum(hot.astype(jnp.int32) * (lid[None, :] + 1), axis=1) - 1
            return hot.astype(BF16), rows, jnp.concatenate([lids, jnp.full((128,), case, jnp.int32)])

        cross_hot, send_x, send_lid = place(cross, hidden)
        send_x, rows, bg0_cut, bu0_cut = lax.optimization_barrier((send_x, hidden, bg0, bu0))
        recv_x = lax.ppermute(send_x, 'data', to_chip)
        recv_lid = lax.ppermute(send_lid, 'data', to_chip)
        cuts = [b[:, :early * BLOCK] for b in (bg0_cut, bu0_cut)]
        bg1_early, bu1_early = (lax.ppermute(b, 'data', to_core) for b in cuts)
        stay_hot, stay_x, stay_lid = place(~cross, rows)

        def low(x, lids):
            info = jnp.stack([lids[tok], me])
            lid_rows = lids[:tok, None]
            lg, lu = low_rows(info, x, lid_rows, ag, au, own_rows, rank)
            return info, x, lid_rows, lg, lu, w_gate, w_up

        stay = low(stay_x, stay_lid)
        late = lax.optimization_barrier((bg0, bu0, bd0, bg1_early, bu1_early, stay))
        bg1, bu1, bd1 = (lax.ppermute(b, 'data', to_core) for b in late[:3])
        bg1_early, bu1_early, stay = late[3:]
        b_all = [(bg0, False), (bg1, False), (bu0, False), (bu1, False)]
        b_early = [(bg0, False), (bg1_early, True), (bu0, False), (bu1_early, True)]
        b_out = [bd0, bd1]
        sums = mlp(*stay, b_early, w_down, ad, None, rank, 0, early)
        recv_x, recv_lid, sums = lax.optimization_barrier((recv_x, recv_lid, sums))
        recv_y = mlp(*low(recv_x, recv_lid), b_all, w_down, ad, b_out, rank, 0, blocks)
        back_y = lax.ppermute(recv_y, 'data', to_chip)
        recv_y, sums = lax.optimization_barrier((recv_y, sums))
        stay_y = mlp(*stay, b_all, w_down, ad, b_out, rank, early, blocks, sums)

        pick = (((0,), (0,)), ((), ()))
        out = lax.dot_general(stay_hot, stay_y, pick, preferred_element_type=F32)
        out += lax.dot_general(cross_hot, back_y, pick, preferred_element_type=F32)
        return out.astype(BF16)

    return jax.shard_map(device_fn, mesh=mesh, in_specs=(row_spec, tok_spec, full_two, full_two, full_two, full_three, owned, full_three, owned, full_three, owned), out_specs=row_spec, check_vma=False)
```

```python
import functools

import jax
import jax.numpy as jnp
from jax import lax
from jax.experimental import pallas as pl
from jax.experimental.pallas import tpu as pltpu
from jax.sharding import PartitionSpec as P


LORA_SCALE = 2.0
F32 = jnp.float32
BF16 = jnp.bfloat16
NT = (((1,), (1,)), ((), ()))
VMEM_LIMIT = 62 * 1024 * 1024
BLOCK = 512


def row_cases(tok):
    if tok == 512:
        return ((256, 352), (96, 352), (256, 368), (112, 368), (256, 512))
    return ((tok // 2, tok),)


def per_case(info_ref, tok, body):
    for index, (split, rows) in enumerate(row_cases(tok)):
        pl.when(info_ref[0] == index)(functools.partial(body, split, rows))


def whole(shape):
    zeros = (0,) * len(shape)
    return pl.BlockSpec(shape, lambda *_: zeros, pipeline_mode=pl.Buffered(1))


def low_kernel(rank, info_ref, x_ref, lid_ref, ag0_ref, ag1_ref, au0_ref, au1_ref, lg_ref, lu_ref):
    width = ag0_ref.shape[0]
    block = pl.program_id(0)

    def body(split, m):
        def masked(rows, a_ref):
            low = lax.dot_general(x_ref[rows, :], a_ref[...], NT, preferred_element_type=F32)
            column = block * width + lax.broadcasted_iota(jnp.int32, low.shape, 1)
            return jnp.where((column // rank) == lid_ref[rows, :], low, 0.0).astype(BF16)

        for a0_ref, a1_ref, l_ref in ((ag0_ref, ag1_ref, lg_ref), (au0_ref, au1_ref, lu_ref)):
            l_ref[:split, :] = masked(slice(0, split), a0_ref)
            l_ref[split:m, :] = masked(slice(split, m), a1_ref)

    per_case(info_ref, x_ref.shape[0], body)


def low_rows(info, x, lid, ag, au, own_rows, rank):
    tok, d = x.shape
    width = own_rows // 2
    spec_a = [pl.BlockSpec((width, d), lambda b, info, side=side: ((info[1] ^ side) * 2 + b, 0)) for side in (0, 1)]
    spec_l = pl.BlockSpec((tok, width), lambda b, info: (0, b))
    return pl.pallas_call(
        functools.partial(low_kernel, rank),
        grid_spec=pltpu.PrefetchScalarGridSpec(
            num_scalar_prefetch=1,
            grid=(2,),
            in_specs=[whole((tok, d)), whole((tok, 1)), *spec_a, *spec_a],
            out_specs=[spec_l, spec_l],
        ),
        out_shape=[jax.ShapeDtypeStruct((tok, own_rows), BF16)] * 2,
        compiler_params=pltpu.CompilerParams(vmem_limit_bytes=VMEM_LIMIT),
        cost_estimate=pl.CostEstimate(flops=4 * tok * d * own_rows, bytes_accessed=8 * own_rows * d, transcendentals=0),
    )(info, x, lid, ag, ag, au, au)


def mlp_kernel(rank, sub, wide, resume, final, begin, info_ref, x_ref, lid_ref, lg_ref, lu_ref, wg_ref, wu_ref, bg0_ref, bg1_ref,
               bu0_ref, bu1_ref, wd_ref, a0_ref, a1_ref, *refs):
    refs = list(refs)
    bd0_ref, bd1_ref = (refs.pop(0), refs.pop(0)) if final else (None, None)
    acc_in, low_in = (refs.pop(0), refs.pop(0)) if resume else (None, None)
    o_ref = refs.pop(0) if final else None
    acc_out, low_out = (None, None) if final else (refs.pop(0), refs.pop(0))
    acc_ref, low_ref, ld_ref, sems, ring_ref, ring_sems = refs
    step = pl.program_id(0)
    tok, d = acc_ref.shape
    half = bg0_ref.shape[0]
    block = bg0_ref.shape[1]
    parts = block // sub
    steps = pl.num_programs(0)
    base_slot = (step % 2) * parts

    def ring_copies(part, slot):
        at = pl.ds(pl.multiple_of(begin + part * sub, sub), sub)
        return [pltpu.make_async_copy(w_ref.at[:, at], ring_ref.at[i, slot], ring_sems.at[i, slot]) for i, w_ref in enumerate((wg_ref, wu_ref))]

    @pl.when(step == 0)
    def _():
        for slot in range(2 * parts):
            for copy in ring_copies(jnp.minimum(slot, steps * parts - 1), slot):
                copy.start()

    for part in range(parts):
        for copy in ring_copies(part, base_slot + part):
            copy.wait()

    def move(pairs):
        copies = [pltpu.make_async_copy(src, dst, sems.at[i]) for i, (src, dst) in enumerate(pairs)]
        for copy in copies:
            copy.start()
        for copy in copies:
            copy.wait()

    def body(split, m):
        def spread(l_ref, at, b0_ref, b1_ref):
            own = jnp.dot(l_ref[:split, :], b0_ref[:, at], preferred_element_type=F32)
            partner = jnp.dot(l_ref[split:m, :], b1_ref[:, at], preferred_element_type=F32)
            return (LORA_SCALE * jnp.concatenate([own, partner], axis=0)).astype(BF16).astype(F32)

        def branch(at, kind, l_ref, b0_ref, b1_ref):
            weight = ring_ref[kind, base_slot + at.start // sub]
            base = jnp.dot(x_ref[:m, :], weight, preferred_element_type=F32)
            return base + spread(l_ref, at, b0_ref, b1_ref)

        @pl.when(step == 0)
        def _():
            if resume:
                move(((acc_in, acc_ref), (low_in, low_ref)))
            else:
                acc_ref[:m, :] = jnp.zeros((m, d), F32)
                low_ref[:m, :] = jnp.zeros((m, half), F32)

        def gate_up(at):
            return at, branch(at, 0, lg_ref, bg0_ref, bg1_ref), branch(at, 1, lu_ref, bu0_ref, bu1_ref)

        def add_down(at, gate, up):
            h = (jax.nn.silu(gate) * up).astype(BF16)
            for rows, a_ref in ((slice(0, split), a0_ref), (slice(split, m), a1_ref)):
                low_ref[rows, :] += lax.dot_general(h[rows, :], a_ref[:, at], NT, preferred_element_type=F32)
            for left in range(0, d, wide):
                to = slice(left, left + wide)
                acc_ref[:m, to] += jnp.dot(h, wd_ref[at, to], preferred_element_type=F32)

        waiting = None
        for first in range(0, block, sub):
            now = gate_up(slice(first, first + sub))
            if first + sub == block:
                for part in range(parts):
                    following = jnp.minimum((step + 2) * parts + part, steps * parts - 1)
                    for copy in ring_copies(following, base_slot + part):
                        copy.start()
            if waiting is not None:
                add_down(*waiting)
            waiting = now
        add_down(*waiting)

        @pl.when(step == pl.num_programs(0) - 1)
        def _():
            if not final:
                move(((acc_ref, acc_out), (low_ref, low_out)))
                return
            column = lax.broadcasted_iota(jnp.int32, (m, half), 1)
            mine = (column // rank) == lid_ref[:m, :]
            ld_ref[:m, :] = jnp.where(mine, low_ref[:m, :], 0.0).astype(BF16)

            def finish(i, carry):
                to = pl.ds(pl.multiple_of(i * wide, wide), wide)
                down = acc_ref[:m, to] + spread(ld_ref, to, bd0_ref, bd1_ref)
                o_ref[:m, to] = (x_ref[:m, to].astype(F32) + down).astype(BF16)
                return carry

            lax.fori_loop(0, d // wide, finish, 0)
            if m < tok:
                o_ref[m:, :] = jnp.zeros((tok - m, d), BF16)

    per_case(info_ref, tok, body)

    @pl.when(step == steps - 1)
    def _():
        for slot in range(2 * parts):
            for copy in ring_copies(slot, slot):
                copy.wait()


def mlp(info, x, lid, lg, lu, wg, wu, bs, wd, ad, bd, rank, first, stop, sums=None, block=BLOCK, sub=256, wide=512):
    tok, d = x.shape
    low = half = lg.shape[1]
    resume, final = sums is not None, bd is not None
    any_spec = pl.BlockSpec(memory_space=pl.ANY)
    in_specs = [
        whole((tok, d)), whole((tok, 1)), whole((tok, low)), whole((tok, low)), any_spec, any_spec,
        *(pl.BlockSpec((half, block), lambda i, info, off=0 if local else first: (0, i + off)) for _, local in bs),
        pl.BlockSpec((block, d), lambda i, info: (i + first, 0)),
        pl.BlockSpec((half, block), lambda i, info: (info[1], i + first)),
        pl.BlockSpec((half, block), lambda i, info: (info[1] ^ 1, i + first)),
    ]
    args = [x, lid, lg, lu, wg, wu, *(b for b, _ in bs), wd, ad, ad]
    if final:
        in_specs += [whole((half, d))] * 2
        args += bd
        out_specs, out_shape = whole((tok, d)), jax.ShapeDtypeStruct((tok, d), BF16)
    else:
        out_specs = [any_spec] * 2
        out_shape = [jax.ShapeDtypeStruct((tok, d), F32), jax.ShapeDtypeStruct((tok, low), F32)]
    if resume:
        in_specs += [any_spec] * 2
        args += sums
    width = (stop - first) * block
    return pl.pallas_call(
        functools.partial(mlp_kernel, rank, sub, wide, resume, final, first * block),
        grid_spec=pltpu.PrefetchScalarGridSpec(
            num_scalar_prefetch=1,
            grid=(stop - first,),
            in_specs=in_specs,
            out_specs=out_specs,
            scratch_shapes=[pltpu.VMEM((tok, d), F32), pltpu.VMEM((tok, low), F32), pltpu.VMEM((tok, low), BF16), pltpu.SemaphoreType.DMA((2,)), pltpu.VMEM((2, 2 * (block // sub), d, sub), BF16), pltpu.SemaphoreType.DMA((2, 2 * (block // sub)))],
        ),
        out_shape=out_shape,
        compiler_params=pltpu.CompilerParams(vmem_limit_bytes=VMEM_LIMIT),
        cost_estimate=pl.CostEstimate(flops=6 * tok * (d + low) * width if final else 1000, bytes_accessed=6 * width * (d + low), transcendentals=tok * width),
    )(info, *args)


def solution(mesh):
    groups = mesh.shape['data']
    assert groups == 4
    row_spec = P(('rep', 'data'), None)
    tok_spec = P(('rep', 'data'))
    full_two = P(None, None)
    full_three = P(None, None, None)
    owned = P('data', None, None)
    to_chip = [(j, j ^ 2) for j in range(groups)]
    to_core = [(j, j ^ 1) for j in range(groups)]

    def device_fn(hidden, adapter_id, w_gate, w_up, w_down, a_gate, b_gate, a_up, b_up, a_down, b_down):
        tok, _ = hidden.shape
        adapters, f, rank = a_down.shape
        per_owner = b_gate.shape[0]
        own_rows = per_owner * rank
        me = lax.axis_index('data').astype(jnp.int32)

        blocks = f // BLOCK
        early = max(1, blocks // 4)

        bg0, bu0, bd0 = (b.reshape(own_rows, b.shape[2]) for b in (b_gate, b_up, b_down))
        ag, au, ad = (jnp.transpose(a, (0, 2, 1)).reshape(adapters * rank, a.shape[1]) for a in (a_gate, a_up, a_down))

        owner = adapter_id // per_owner
        cross = (owner // 2) != (me // 2)
        partner = ((owner ^ me) & 1) == 1
        lid = adapter_id % per_owner
        token = jnp.arange(tok, dtype=jnp.int32)
        before = token[None, :] < token[:, None]

        def place(chosen, hidden):
            own = jnp.sum((chosen & ~partner).astype(jnp.int32))
            other = jnp.sum((chosen & partner).astype(jnp.int32))
            *rest, last = enumerate(row_cases(tok))
            case, split = jnp.int32(last[0]), jnp.int32(last[1][0])
            for index, (first_other, size) in reversed(rest):
                fits = (own <= first_other) & (other <= size - first_other)
                case = jnp.where(fits, index, case)
                split = jnp.where(fits, first_other, split)
            alike = before & chosen[None, :] & (partner[None, :] == partner[:, None])
            rank_of = jnp.sum(alike.astype(jnp.int32), axis=1) + jnp.where(partner, split, 0)
            hot = (token[:, None] == rank_of[None, :]) & chosen[None, :]
            rows = jnp.dot(hot.astype(BF16), hidden, preferred_element_type=F32).astype(BF16)
            lids = jnp.sum(hot.astype(jnp.int32) * (lid[None, :] + 1), axis=1) - 1
            return hot.astype(BF16), rows, jnp.concatenate([lids, jnp.full((128,), case, jnp.int32)])

        cross_hot, send_x, send_lid = place(cross, hidden)
        send_x, rows, bg0_cut, bu0_cut = lax.optimization_barrier((send_x, hidden, bg0, bu0))
        recv_x = lax.ppermute(send_x, 'data', to_chip)
        recv_lid = lax.ppermute(send_lid, 'data', to_chip)
        cuts = [b[:, :early * BLOCK] for b in (bg0_cut, bu0_cut)]
        bg1_early, bu1_early = (lax.ppermute(b, 'data', to_core) for b in cuts)
        stay_hot, stay_x, stay_lid = place(~cross, rows)

        def low(x, lids):
            info = jnp.stack([lids[tok], me])
            lid_rows = lids[:tok, None]
            lg, lu = low_rows(info, x, lid_rows, ag, au, own_rows, rank)
            return info, x, lid_rows, lg, lu, w_gate, w_up

        stay = low(stay_x, stay_lid)
        late = lax.optimization_barrier((bg0, bu0, bd0, bg1_early, bu1_early, stay))
        bg1, bu1, bd1 = (lax.ppermute(b, 'data', to_core) for b in late[:3])
        bg1_early, bu1_early, stay = late[3:]
        b_all = [(bg0, False), (bg1, False), (bu0, False), (bu1, False)]
        b_early = [(bg0, False), (bg1_early, True), (bu0, False), (bu1_early, True)]
        b_out = [bd0, bd1]
        sums = mlp(*stay, b_early, w_down, ad, None, rank, 0, early)
        recv_x, recv_lid, sums = lax.optimization_barrier((recv_x, recv_lid, sums))
        recv_y = mlp(*low(recv_x, recv_lid), b_all, w_down, ad, b_out, rank, 0, blocks)
        back_y = lax.ppermute(recv_y, 'data', to_chip)
        recv_y, sums = lax.optimization_barrier((recv_y, sums))
        stay_y = mlp(*stay, b_all, w_down, ad, b_out, rank, early, blocks, sums)

        pick = (((0,), (0,)), ((), ()))
        out = lax.dot_general(stay_hot, stay_y, pick, preferred_element_type=F32)
        out += lax.dot_general(cross_hot, back_y, pick, preferred_element_type=F32)
        return out.astype(BF16)

    return jax.shard_map(device_fn, mesh=mesh, in_specs=(row_spec, tok_spec, full_two, full_two, full_two, full_three, owned, full_three, owned, full_three, owned), out_specs=row_spec, check_vma=False)
```
